32 devices in a mesh: client: 32 (over z, y, x, core).
Axes of the slice: x: 2, y: 2, z: 4, core: 2. Of those that a mesh axis runs over, the one named last changes fastest.
Arguments:
- patches: bfloat16 [4096, 192], P('client'), may hold values from -6 to 6
- labels: int32 [256], replicated, may hold values from 0 to 9
- assign: int32 [32, 1], replicated, may hold values from 0 to 15; in each aligned block of 32 rows (0 to 31, 32 to 63, ...) at most 4 rows name the same one
- patch_embed: bfloat16 [192, 384], replicated, may hold values from -0.4375 to 0.4375
- positions: bfloat16 [16, 384], replicated, may hold values from -3 to 3
- client_in: bfloat16 [384, 3072], replicated, may hold values from -3 to 3
- client_down: bfloat16 [1536, 384], replicated, may hold values from -0.15625 to 0.15625
- server_in: bfloat16 [2, 6144, 3072], P(None, 'client'), may hold values from -3 to 3
- server_down: bfloat16 [2, 24576, 384], P(None, 'client'), may hold values from -0.15625 to 0.15625
- classifier: bfloat16 [16, 384, 10], replicated, may hold values from -15 to 15
Outputs:
- losses: float32 [32, 16], P('client')
- grad_patch_embed: float32 [192, 384], P(None, 'client')
- grad_positions: float32 [16, 384], P(None, 'client')
- grad_client_in: float32 [384, 3072], P(None, 'client')
- grad_client_down: float32 [1536, 384], P(None, 'client')
- grad_server_in: float32 [2, 6144, 3072], P(None, 'client')
- grad_server_down: float32 [2, 24576, 384], P(None, 'client')
- grad_classifier: float32 [6144, 10], P('client')
The draws below stay inside these ranges and needn't reach their ends.
Inputs may be any that keep to these rules, and one draw needn't show every extreme that they name: `assign`: no server shard is named by more than 4 clients, a bound that some block reaches.
All inputs are finite; a program needn't handle non-finite values.
Results may differ from the reference program's by a relative error of at most 0.025.
Values may be sent and summed in bfloat16 or wider, within the bound.
A program may use at most 128 MiB of HBM per device.

```python
import math
import jax
import jax.numpy as jnp
import numpy as np
from jax import lax

D = 384
HEADS = 6
FF = 1536
PATCH = 192
TOK = 16
CLASSES = 10
IMG = 8
SHARDS = 16
SLOTS = 2
SERVER_LAYERS = 2
CAPACITY = 4
N_CLIENT = 32


def scaled_normal(key, shape, fan_in):
    return jax.random.truncated_normal(key, -4.0, 4.0, shape, jnp.float32) / math.sqrt(fan_in)


def draw_client_in(key, part):
    values = scaled_normal(jax.random.fold_in(key, 11), (D, 4 * D + FF), D)
    return values.astype(jnp.bfloat16)


def draw_server_in(key, part):
    values = scaled_normal(jax.random.fold_in(key, 23), (SERVER_LAYERS, SHARDS * D, 4 * D + FF), D)
    return values.astype(jnp.bfloat16)


def draw_classifier(key, part):
    values = scaled_normal(jax.random.fold_in(key, 37), (SHARDS, D, CLASSES), D)
    return values.astype(jnp.bfloat16)


def place_ends(result, key, least, high):
    dims = result.shape
    place = [jax.random.randint(jax.random.fold_in(key, axis), (), 0, dims[axis]) for axis in range(len(dims))]
    result = result.at[tuple(place)].set(least)
    longest = dims.index(max(dims))
    place[longest] = (place[longest] + 1) % dims[longest]
    return result.at[tuple(place)].set(high)


def levels(key, extent, split, least, top_value):
    level, own = 1.0, jax.random.fold_in(key, 6)
    for dim, blocks in split:
        steps = jnp.exp(jax.random.uniform(jax.random.fold_in(own, dim), (blocks,), jnp.float32, least / len(split), top_value / len(split)))
        level = level * jnp.repeat(steps, extent[dim] // blocks).reshape([-1 if axis == dim else 1 for axis in range(len(extent))])
    return level


def assign_block(stream_key, own, number, rows, amount, top, reach, lean):
    sequence = jax.random.permutation(stream_key, amount)
    heavy_load, common = shares(amount, rows * top, reach, lean, True), shares(amount, rows * top, reach, lean, False)
    places = jnp.arange(amount)

    def named(sizes, rotation):
        used = int((sizes > 0).sum())
        fixed = max(1, used // 4)
        shifted = fixed + (places - fixed + rotation * (used - fixed)) % max(1, amount - fixed)
        return jnp.zeros((amount,), jnp.int32).at[sequence[jnp.where(places < fixed, places, shifted)]].set(jnp.asarray(sizes, jnp.int32))

    sizes = jnp.where(number % 4 == 0, named(heavy_load, number // 4), named(common, number - number // 4 - 1))
    mixed = jax.random.permutation(jax.random.fold_in(own, 3), amount)
    donor, sink = mixed[0:amount // 2 * 2:2], mixed[1:amount // 2 * 2:2]
    margin = jnp.minimum(sizes[donor] - 1, reach - sizes[sink]) // 2
    margin = jnp.where((donor == sequence[0]) | (sink == sequence[0]) | (sizes[sink] == 0), 0, jnp.maximum(margin, 0))
    shifted = jax.random.randint(jax.random.fold_in(own, 4), (amount // 2,), 0, 1 << 20) % (margin + 1)
    sizes = sizes.at[donor].add(-shifted).at[sink].add(shifted)
    items = jnp.searchsorted(jnp.cumsum(sizes), jnp.arange(rows * top), side="right").astype(jnp.int32)
    grid = items.reshape(top, rows).T
    grid = grid[jax.random.permutation(jax.random.fold_in(own, 1), rows)]
    rotation = jax.random.randint(jax.random.fold_in(own, 2), (rows, 1), 0, top)
    return jnp.take_along_axis(grid, (jnp.arange(top)[None, :] + rotation) % top, axis=1)


def shares(count, total, reach, slope, full):
    weights = [(1 << 20) // math.isqrt(rank ** slope) + 1 for rank in range(1, count + 1)]
    largest = reach if full else min(reach, max(-(-total // count), total * weights[0] // sum(weights)))
    least = 1 if total - largest >= count - 1 else 0
    given, spare = [largest] + [least] * (count - 1), total - largest - least * (count - 1)
    while spare > 0:
        candidates = [i for i in range(1, count) if given[i] < largest] or [i for i in range(1, count) if given[i] < reach]
        mass, remaining = sum([weights[i] for i in candidates]), spare
        for i in candidates:
            addition = min(reach - given[i], max(1, remaining * weights[i] // mass), spare)
            given[i] = given[i] + addition
            spare = spare - addition
    return np.array(given)


def normal_values(rng, extent, scale, bound, cuts=(), kind=jnp.bfloat16):
    entries = jax.random.normal(rng, extent, jnp.float32) * scale
    if len(cuts) > 0:
        entries = levels(rng, extent, cuts, -0.22, 0.18) * entries
    return jnp.clip(entries, min=-bound, max=bound).astype(kind)


def setup_inputs(seed: int = 0) -> dict:
    splits = jax.random.split(jax.random.key(seed), 11)
    patches = normal_values(splits[0], (N_CLIENT * IMG * TOK, PATCH), 1.0, 6.0, ((0, 32),))
    labels = place_ends(jax.random.randint(splits[1], (N_CLIENT * IMG,), 0, CLASSES), jax.random.fold_in(splits[1], 1), 0, CLASSES - 1).astype(jnp.int32)
    assign_keys = jax.random.split(jax.random.fold_in(splits[2], 1), N_CLIENT // N_CLIENT)
    assign_turns = jax.random.permutation(jax.random.fold_in(splits[2], 3), N_CLIENT // N_CLIENT)
    assign = jax.vmap(lambda own, number: assign_block(jax.random.fold_in(splits[2], 2), own, number, N_CLIENT, SHARDS, 1, CAPACITY, 2))(assign_keys, assign_turns).reshape((N_CLIENT, 1))
    patch_embed = normal_values(splits[3], (PATCH, D), PATCH ** -0.5, 0.4375)
    positions = normal_values(splits[4], (TOK, D), 0.5, 3.0)
    client_in = draw_client_in(jax.random.fold_in(splits[10], 71), 0)
    client_down = normal_values(splits[6], (FF, D), FF ** -0.5, 0.15625)
    server_in = draw_server_in(jax.random.fold_in(splits[10], 71), 0)
    server_down = normal_values(splits[8], (SERVER_LAYERS, SHARDS * FF, D), FF ** -0.5, 0.15625, ((1, 32),))
    classifier = draw_classifier(jax.random.fold_in(splits[10], 71), 0)
    return dict(patches=patches, labels=labels, assign=assign, patch_embed=patch_embed, positions=positions, client_in=client_in, client_down=client_down, server_in=server_in, server_down=server_down, classifier=classifier)


EPSILON = 1e-06

def layer_norm(inputs):
    centre = inputs - lax.optimization_barrier(jnp.mean(inputs, axis=-1, keepdims=True))
    spread = lax.optimization_barrier(jnp.mean(centre * centre, axis=-1, keepdims=True))
    return centre * lax.rsqrt(spread + EPSILON)

def encoder_block(stream, weight_in, weight_down):
    images, tokens, model_width = stream.shape
    head_dim = model_width // HEADS
    normed = layer_norm(stream).astype(jnp.bfloat16).reshape(images * tokens, model_width)
    projected = jnp.dot(normed, weight_in[:, :3 * model_width], preferred_element_type=jnp.float32)
    projected = projected.reshape(images, tokens, 3, HEADS, head_dim)
    queries = projected[:, :, 0]
    key_rows = projected[:, :, 1]
    values = projected[:, :, 2]
    scores = jnp.einsum('bqhe,bkhe->bhqk', queries, key_rows, precision=lax.Precision.HIGHEST) / math.sqrt(head_dim)
    weights_attn = jax.nn.softmax(scores, axis=-1)
    attended = jnp.einsum('bhqk,bkhe->bqhe', weights_attn, values, precision=lax.Precision.HIGHEST)
    attended = attended.reshape(images * tokens, model_width).astype(jnp.bfloat16)
    stream = stream + jnp.dot(attended, weight_in[:, 3 * model_width:4 * model_width], preferred_element_type=jnp.float32).reshape(images, tokens, model_width)
    normed = layer_norm(stream).astype(jnp.bfloat16).reshape(images * tokens, model_width)
    hidden = jax.nn.gelu(jnp.dot(normed, weight_in[:, 4 * model_width:], preferred_element_type=jnp.float32)).astype(jnp.bfloat16)
    return stream + jnp.dot(hidden, weight_down, preferred_element_type=jnp.float32).reshape(images, tokens, model_width)

def client_forward(patch_rows, patch_embed, positions, client_in, client_down):
    stream = jnp.dot(patch_rows, patch_embed, preferred_element_type=jnp.float32).reshape(-1, TOK, D)
    stream = stream + positions.astype(jnp.float32)
    stream = encoder_block(stream, client_in, client_down)
    return stream.reshape(-1, D).astype(jnp.bfloat16)

def server_loss(cut_rows, slot_hot, weights_in, weights_down, class_shard):
    stream = cut_rows.astype(jnp.float32).reshape(-1, TOK, D)
    for layer in range(len(weights_in)):
        stream = encoder_block(stream, weights_in[layer], weights_down[layer])
    pooled = layer_norm(lax.optimization_barrier(jnp.mean(stream, axis=1))).astype(jnp.bfloat16)
    logits = jnp.dot(pooled, class_shard, preferred_element_type=jnp.float32)
    per_loss = (jax.nn.logsumexp(logits, axis=-1) - lax.optimization_barrier(jnp.sum(slot_hot * logits, axis=-1))) * lax.optimization_barrier(jnp.sum(slot_hot, axis=-1))
    return (jnp.sum(per_loss), per_loss)

def arrival_rank(routes):
    places = jnp.arange(routes.shape[0], dtype=jnp.int32)
    earlier = (routes[:, None] == routes[None, :]) & (places[:, None] < places[None, :])
    return lax.optimization_barrier(jnp.sum(earlier.astype(jnp.int32), axis=0))

def select_matrix(routes, arrival, shard, capacity):
    slots_here = jnp.arange(capacity, dtype=jnp.int32)[:, None]
    return ((routes[None, :] == shard) & (arrival[None, :] == slots_here)).astype(jnp.bfloat16)

def slot_labels(labels, selector, rank_in_group, per_image, members):
    label_table = labels.reshape(members, IMG)
    label_part = lax.dynamic_slice_in_dim(label_table, (rank_in_group * per_image).astype(jnp.int32), per_image, 1)
    onehot = (label_part[:, :, None] == jnp.arange(CLASSES, dtype=jnp.int32)[None, None, :]).astype(jnp.float32)
    onehot = onehot.reshape(members, per_image * CLASSES)
    chosen = jnp.dot(selector.astype(jnp.float32), onehot, precision=lax.Precision.HIGHEST)
    return chosen.reshape(-1, CLASSES)

def reference(patches, labels, assign, patch_embed, positions, client_in, client_down, server_in, server_down, classifier):
    members = N_CLIENT
    group_size = members // SHARDS
    per_image = IMG // group_size
    piece_rows = IMG * TOK // group_size
    capacity = SLOTS * group_size
    width_all = 4 * D + FF
    routes = assign[:, 0]
    arrival = arrival_rank(routes)
    patch_sets = patches.reshape(members, IMG * TOK, PATCH)

    def client_cut(patch_rows):
        return client_forward(patch_rows, patch_embed, positions, client_in, client_down)
    cuts = lax.map(client_cut, patch_sets)
    cut_pieces = cuts.reshape(members, group_size, piece_rows * D)
    shard_in = server_in.reshape(SERVER_LAYERS, SHARDS, D, width_all)
    shard_down = server_down.reshape(SERVER_LAYERS, SHARDS, FF, D)

    def device_step(carry, device):
        acc_in, acc_down, acc_class = carry
        shard = device // group_size
        rank_in_group = device % group_size
        selector = select_matrix(routes, arrival, shard, capacity)
        own_piece = lax.dynamic_index_in_dim(cut_pieces, rank_in_group, 1, keepdims=False)
        compact = jnp.dot(selector, own_piece, preferred_element_type=jnp.float32).astype(jnp.bfloat16)
        compact = compact.reshape(capacity * piece_rows, D)
        slot_hot = slot_labels(labels, selector, rank_in_group, per_image, members)
        layer_in = lax.dynamic_index_in_dim(shard_in, shard, 1, keepdims=False)
        layer_down = lax.dynamic_index_in_dim(shard_down, shard, 1, keepdims=False)
        class_shard = lax.dynamic_index_in_dim(classifier, shard, 0, keepdims=False)

        def loss_of(cut_rows, weights_in, weights_down, class_weights):
            return server_loss(cut_rows, slot_hot, weights_in, weights_down, class_weights)
        list_in = tuple((layer_in[layer] for layer in range(SERVER_LAYERS)))
        list_down = tuple((layer_down[layer] for layer in range(SERVER_LAYERS)))
        total_loss, server_back, per_loss = jax.vjp(loss_of, compact, list_in, list_down, class_shard, has_aux=True)
        grad_cut, grad_in, grad_down, grad_class = server_back(jnp.ones((), jnp.float32))
        acc_in = acc_in.at[:, shard].add(jnp.stack(grad_in).astype(jnp.float32))
        acc_down = acc_down.at[:, shard].add(jnp.stack(grad_down).astype(jnp.float32))
        acc_class = acc_class.at[shard].add(grad_class.astype(jnp.float32))
        return ((acc_in, acc_down, acc_class), (grad_cut, per_loss))
    start = (jnp.zeros((SERVER_LAYERS, SHARDS, D, width_all), jnp.float32), jnp.zeros((SERVER_LAYERS, SHARDS, FF, D), jnp.float32), jnp.zeros((SHARDS, D, CLASSES), jnp.float32))
    sums, outputs = lax.scan(device_step, start, jnp.arange(members, dtype=jnp.int32))
    acc_in, acc_down, acc_class = sums
    cut_grads, loss_rows = outputs
    cut_grads = cut_grads.reshape(SHARDS, group_size, capacity, piece_rows * D)

    def client_step(carry, client):
        shard = routes[client]
        slot = arrival[client]
        by_shard = lax.dynamic_index_in_dim(cut_grads, shard, 0, keepdims=False)
        own_grads = lax.dynamic_index_in_dim(by_shard, slot, 1, keepdims=False).reshape(IMG * TOK, D)
        patch_rows = lax.dynamic_index_in_dim(patch_sets, client, 0, keepdims=False)

        def client_of(embed_weights, position_weights, in_weights, down_weights):
            return client_forward(patch_rows, embed_weights, position_weights, in_weights, down_weights)
        cut_again, client_back = jax.vjp(client_of, patch_embed, positions, client_in, client_down)
        grads = client_back(own_grads)
        return (tuple((total + part_grad.astype(jnp.float32) for total, part_grad in zip(carry, grads))), None)
    client_start = (jnp.zeros((PATCH, D), jnp.float32), jnp.zeros((TOK, D), jnp.float32), jnp.zeros((D, width_all), jnp.float32), jnp.zeros((FF, D), jnp.float32))
    client_sums, unused = lax.scan(client_step, client_start, jnp.arange(members, dtype=jnp.int32))
    return (loss_rows, client_sums[0], client_sums[1], client_sums[2], client_sums[3], acc_in.reshape(SERVER_LAYERS, SHARDS * D, width_all), acc_down.reshape(SERVER_LAYERS, SHARDS * FF, D), acc_class.reshape(SHARDS * D, CLASSES))
```

```python
import functools
import math

import jax
import jax.numpy as jnp
from jax import lax
from jax.experimental import pallas as pl
from jax.experimental.pallas import tpu as pltpu
from jax.sharding import PartitionSpec as P

HEADS = 6
TOK = 16
IMG = 8
SHARDS = 16
SLOTS = 2
EPSILON = 1e-06
LANES = 128
PAD = 16
BF = jnp.bfloat16
F32 = jnp.float32
HIGH = lax.Precision.HIGHEST
GELU_C = math.sqrt(2.0 / math.pi)
VMEM_LIMIT = 60 * 1024 * 1024
MESH = pl.DeviceIdType.MESH


def mm(a, b, precision=None):
    return lax.dot_general(
        a, b, (((1,), (0,)), ((), ())), precision=precision, preferred_element_type=F32
    )


def mm_nt(a, b, precision=None):
    return lax.dot_general(
        a, b, (((1,), (1,)), ((), ())), precision=precision, preferred_element_type=F32
    )


def mm_tn(a, b):
    return lax.dot_general(a, b, (((0,), (0,)), ((), ())), preferred_element_type=F32)


def norm(v):
    centre = v - jnp.mean(v, axis=-1, keepdims=True)
    scale = lax.rsqrt(jnp.mean(centre * centre, axis=-1, keepdims=True) + EPSILON)
    return centre * scale, scale


def norm_back(normed, scale, grad):
    return scale * (
        grad
        - jnp.mean(grad, axis=-1, keepdims=True)
        - normed * jnp.mean(grad * normed, axis=-1, keepdims=True)
    )


def gelu(v):
    t = jnp.tanh(GELU_C * (v + 0.044715 * (v * v * v)))
    return 0.5 * v * (1.0 + t)


def gelu_both(v):
    sq = v * v
    t = jnp.tanh(GELU_C * (v + 0.044715 * (sq * v)))
    value = 0.5 * v * (1.0 + t)
    slope = 0.5 * (1.0 + t) + 0.5 * v * (1.0 - t * t) * (GELU_C * (1.0 + 0.134145 * sq))
    return value, slope


def image_mask():
    row = lax.broadcasted_iota(jnp.int32, (LANES, LANES), 0)
    col = lax.broadcasted_iota(jnp.int32, (LANES, LANES), 1)
    return row // TOK == col // TOK


def lane_masks(head_dim):
    lane = lax.broadcasted_iota(jnp.int32, (LANES, LANES), 1)
    return [lane // head_dim == h for h in range(LANES // head_dim)]


def attend(qkv_ref, probs_ref, att_ref, width):
    rows = qkv_ref.shape[0]
    head_dim = width // HEADS
    per = LANES // head_dim
    inside = image_mask()
    keeps = lane_masks(head_dim)
    for group in range(rows // LANES):
        r = slice(group * LANES, (group + 1) * LANES)
        for pair in range(width // LANES):
            lo = pair * LANES
            q = qkv_ref[r, lo : lo + LANES]
            k = qkv_ref[r, width + lo : width + lo + LANES]
            v = qkv_ref[r, 2 * width + lo : 2 * width + lo + LANES]
            out = jnp.zeros((LANES, LANES), F32)
            for h in range(per):
                s = mm_nt(jnp.where(keeps[h], q, 0.0), k, HIGH) * (1.0 / math.sqrt(head_dim))
                s = jnp.where(inside, s, -1e30)
                e = jnp.exp(s - jnp.max(s, axis=-1, keepdims=True))
                p = (e / jnp.sum(e, axis=-1, keepdims=True)).astype(BF)
                probs_ref[group * HEADS + pair * per + h] = p
                out = out + mm(p, jnp.where(keeps[h], v, 0.0).astype(BF))
            att_ref[r, lo : lo + LANES] = out.astype(BF)


def attend_back(grad, qkv_ref, probs_ref, dqkv_ref, width):
    rows = qkv_ref.shape[0]
    head_dim = width // HEADS
    per = LANES // head_dim
    keeps = lane_masks(head_dim)
    for group in range(rows // LANES):
        r = slice(group * LANES, (group + 1) * LANES)
        for pair in range(width // LANES):
            lo = pair * LANES
            q = qkv_ref[r, lo : lo + LANES]
            k = qkv_ref[r, width + lo : width + lo + LANES]
            v = qkv_ref[r, 2 * width + lo : 2 * width + lo + LANES].astype(BF)
            go = grad[r, lo : lo + LANES]
            dq = jnp.zeros((LANES, LANES), F32)
            dk = jnp.zeros((LANES, LANES), F32)
            dv = jnp.zeros((LANES, LANES), F32)
            for h in range(per):
                p = probs_ref[group * HEADS + pair * per + h]
                goh = jnp.where(keeps[h], go, 0.0).astype(BF)
                dp = mm_nt(goh, v)
                dv = dv + mm_tn(p, goh)
                pf = p.astype(F32)
                ds = pf * (dp - jnp.sum(pf * dp, axis=-1, keepdims=True))
                ds = (ds * (1.0 / math.sqrt(head_dim))).astype(BF)
                dq = dq + mm(ds, jnp.where(keeps[h], k, 0.0).astype(BF))
                dk = dk + mm_tn(ds, jnp.where(keeps[h], q, 0.0).astype(BF))
            dqkv_ref[r, lo : lo + LANES] = dq.astype(BF)
            dqkv_ref[r, width + lo : width + lo + LANES] = dk.astype(BF)
            dqkv_ref[r, 2 * width + lo : 2 * width + lo + LANES] = dv.astype(BF)


def block_forward(x, w_ref, d_ref, qkv_ref, probs_ref, att_ref, mid_ref, pre_ref):
    width = x.shape[1]
    u = norm(x)[0].astype(BF)
    qkv_ref[...] = mm(u, w_ref[:, : 3 * width])
    attend(qkv_ref, probs_ref, att_ref, width)
    y = x + mm(att_ref[...], w_ref[:, 3 * width : 4 * width])
    mid_ref[...] = y
    u = norm(y)[0].astype(BF)
    pre_ref[...] = mm(u, w_ref[:, 4 * width :])
    h = gelu(pre_ref[...]).astype(BF)
    return y + mm(h, d_ref[...])


def block_backward(
    g, x, w_ref, d_ref, qkv_ref, probs_ref, att_ref, mid_ref, pre_ref, dqkv_ref, put_in, put_down
):
    width = x.shape[1]
    gb = g.astype(BF)
    h, slope = gelu_both(pre_ref[...])
    put_down(h.astype(BF), gb)
    dpre = (mm_nt(gb, d_ref[...]) * slope).astype(BF)
    y = mid_ref[...]
    u, scale = norm(y)
    put_in(4 * width, u.astype(BF), dpre)
    dy = g + norm_back(u, scale, mm_nt(dpre, w_ref[:, 4 * width :]))
    gb = dy.astype(BF)
    put_in(3 * width, att_ref[...], gb)
    attend_back(
        mm_nt(gb, w_ref[:, 3 * width : 4 * width]), qkv_ref, probs_ref, dqkv_ref, width
    )
    u, scale = norm(x)
    dqkv = dqkv_ref[...]
    put_in(0, u.astype(BF), dqkv)
    return dy + norm_back(u, scale, mm_nt(dqkv, w_ref[:, : 3 * width]))


def client_forward_kernel(
    patch_ref, embed_ref, pos_ref, w_ref, d_ref,
    cut_ref, x_ref, qkv_ref, probs_ref, att_ref, mid_ref, pre_ref,
):
    rows = patch_ref.shape[0]
    x = mm(patch_ref[...], embed_ref[...])
    pos = pos_ref[...].astype(F32)
    x = x + jnp.concatenate([pos] * (rows // TOK), axis=0)
    x_ref[...] = x
    cut_ref[...] = block_forward(
        x, w_ref, d_ref, qkv_ref, probs_ref, att_ref, mid_ref, pre_ref
    ).astype(BF)


def client_backward_kernel(
    n, group,
    assign_ref, back_ref, patch_ref, w_ref, d_ref,
    x_ref, qkv_ref, probs_ref, att_ref, mid_ref, pre_ref,
    pack_ref,
    got, dqkv_ref, sem,
):
    me = lax.axis_index("client")
    shard = assign_ref[me]
    copy = pltpu.make_async_copy(back_ref.at[pl.ds(shard * group, group)], got, sem)
    copy.start()
    rows, width = x_ref.shape
    ff = d_ref.shape[0]
    r_in = w_ref.shape[1] // n
    cols = width // n
    src = lax.broadcasted_iota(jnp.int32, (width, n * PAD), 0)
    dst = lax.broadcasted_iota(jnp.int32, (width, n * PAD), 1)
    place = ((dst // PAD == src // cols) & (dst % PAD == src % cols)).astype(F32).astype(BF)
    tok = (
        lax.broadcasted_iota(jnp.int32, (rows, LANES), 0) % TOK
        == lax.broadcasted_iota(jnp.int32, (rows, LANES), 1)
    ).astype(F32).astype(BF)
    copy.wait()
    g = got[...].astype(F32).reshape(rows, width)
    per_dev = w_ref.shape[1] // n

    def put_in(start, lhs, rhs):
        for c in range(0, rhs.shape[1], width):
            part = mm_tn(rhs[:, c : c + width], lhs)
            j = (start + c) // per_dev
            pack_ref[j : j + width // per_dev, :per_dev, :] = part.reshape(
                width // per_dev, per_dev, width
            ).astype(BF)

    def put_down(h, gb):
        spread = mm(gb, place).astype(BF)
        for q in range(ff // width):
            part = mm_tn(spread, h[:, q * width : (q + 1) * width])
            lo = r_in + q * PAD
            pack_ref[:, lo : lo + PAD, :] = part.reshape(n, PAD, width).astype(BF)

    dx = block_backward(
        g, x_ref[...], w_ref, d_ref, qkv_ref, probs_ref, att_ref, mid_ref, pre_ref,
        dqkv_ref, put_in, put_down,
    )
    spread = mm(dx.astype(BF), place).astype(BF)
    lo = r_in + (ff // width) * PAD
    patch = patch_ref.shape[1]
    pack_ref[:, lo : lo + PAD, :patch] = mm_tn(spread, patch_ref[...]).reshape(
        n, PAD, patch
    ).astype(BF)
    pack_ref[:, lo : lo + PAD, width - LANES :] = mm_tn(spread, tok).reshape(
        n, PAD, LANES
    ).astype(BF)


def server_kernel(
    n, group, layers, per_image, capacity, classes, *refs,
):
    assign_ref, label_ref, arrived_ref, class_ref = refs[:4]
    refs = refs[4:]
    in_pieces, refs = refs[:group], refs[group:]
    down_pieces, refs = refs[:group], refs[group:]
    loss_ref, back_ref, gclass_ref = refs[:3]
    refs = refs[3:]
    gin_out, refs = refs[:group], refs[group:]
    gdown_out, refs = refs[:group], refs[group:]
    (
        wbuf, dbuf, gin, gdown, xs, qkv, probs, att, mid, pre, dqkv, gcur, cut,
        slot_ref, w_sem, g_sem, slot_sem,
    ) = refs
    me = lax.axis_index("client")
    rank = me % group
    shard = me // group
    rows_in = in_pieces[0].shape[1]
    rows_down = down_pieces[0].shape[1]
    piece = arrived_ref.shape[1]

    def weight_copies(layer):
        made = []
        for i in range(group):
            who = rank ^ i
            made.append(pltpu.make_async_copy(
                in_pieces[i].at[layer],
                wbuf.at[layer, pl.ds(pl.multiple_of(who * rows_in, rows_in), rows_in)],
                w_sem.at[layer, 2 * i],
            ))
            made.append(pltpu.make_async_copy(
                down_pieces[i].at[layer],
                dbuf.at[layer, pl.ds(pl.multiple_of(who * rows_down, rows_down), rows_down)],
                w_sem.at[layer, 2 * i + 1],
            ))
        return made

    def grad_copies(layer):
        made = []
        for i in range(group):
            who = rank ^ i
            made.append(pltpu.make_async_copy(
                gin.at[layer, pl.ds(pl.multiple_of(who * rows_in, rows_in), rows_in)],
                gin_out[i].at[layer],
                g_sem.at[layer, 2 * i],
            ))
            made.append(pltpu.make_async_copy(
                gdown.at[layer, pl.ds(pl.multiple_of(who * rows_down, rows_down), rows_down)],
                gdown_out[i].at[layer],
                g_sem.at[layer, 2 * i + 1],
            ))
        return made

    for layer in range(layers):
        for c in weight_copies(layer):
            c.start()

    for k in range(capacity):
        slot_ref[k] = 0

    def scan(c, count):
        hit = assign_ref[c] == shard

        @pl.when(hit)
        def _():
            slot_ref[count] = c

        return count + jnp.where(hit, 1, 0)

    filled = lax.fori_loop(0, n, scan, 0)

    def slot_in(k):
        return pltpu.make_async_copy(
            arrived_ref.at[slot_ref[k]], cut.at[pl.ds(k * piece, piece)], slot_sem.at[k]
        )

    for k in range(capacity):
        @pl.when(k < filled)
        def _():
            slot_in(k).start()

        @pl.when(k >= filled)
        def _():
            cut[k * piece : (k + 1) * piece, :] = jnp.zeros((piece, cut.shape[1]), BF)

    images = capacity * per_image
    row = lax.broadcasted_iota(jnp.int32, (images, LANES), 0)
    lane = lax.broadcasted_iota(jnp.int32, (images, LANES), 1)
    want = jnp.full((images, LANES), -1, jnp.int32)
    for k in range(capacity):
        base = slot_ref[k] * (group * per_image) + rank * per_image
        for j in range(per_image):
            lab = jnp.where(k < filled, label_ref[base + j], -1)
            want = jnp.where(row == k * per_image + j, lab, want)
    hot = (lane == want).astype(F32)
    full = (want[:, :1] >= 0).astype(F32)

    for k in range(capacity):
        @pl.when(k < filled)
        def _():
            slot_in(k).wait()

    xs[0] = cut[...].astype(F32)

    def forward(layer, carry):
        for c in weight_copies(layer):
            c.wait()
        xs[layer + 1] = block_forward(
            xs[layer], wbuf.at[layer], dbuf.at[layer], qkv.at[layer], probs.at[layer],
            att.at[layer], mid.at[layer], pre.at[layer],
        )
        return carry

    lax.fori_loop(0, layers, forward, 0)

    rows = cut.shape[0]
    pool = (
        lax.broadcasted_iota(jnp.int32, (images, rows), 1) // TOK
        == lax.broadcasted_iota(jnp.int32, (images, rows), 0)
    ).astype(F32) * (1.0 / TOK)
    unpool = (
        lax.broadcasted_iota(jnp.int32, (rows, images), 0) // TOK
        == lax.broadcasted_iota(jnp.int32, (rows, images), 1)
    ).astype(F32) * (1.0 / TOK)
    u, scale = norm(mm(pool, xs[layers], HIGH))
    pooled = u.astype(BF)
    logits = mm(pooled, class_ref[...])
    logits = jnp.where(lane < classes, logits, -1e30)
    top = jnp.max(logits, axis=-1, keepdims=True)
    e = jnp.exp(logits - top)
    total = jnp.sum(e, axis=-1, keepdims=True)
    loss = (
        jnp.log(total) + top - jnp.sum(jnp.where(lane == want, logits, 0.0), axis=-1, keepdims=True)
    ) * full
    eye = (
        lax.broadcasted_iota(jnp.int32, (images, images), 0)
        == lax.broadcasted_iota(jnp.int32, (images, images), 1)
    )
    loss_ref[...] = jnp.sum(jnp.where(eye, loss, 0.0), axis=0, keepdims=True)
    dlog = ((e / total - hot) * full).astype(BF)
    gclass_ref[...] = mm_tn(pooled, dlog).astype(BF)
    dpool = norm_back(u, scale, mm_nt(dlog, class_ref[...]))
    gcur[...] = mm(unpool, dpool, HIGH)

    def backward(i, carry):
        layer = layers - 1 - i

        def put_in(start, lhs, rhs):
            gin[layer, :, start : start + rhs.shape[1]] = mm_tn(lhs, rhs).astype(BF)

        def put_down(h, gb):
            gdown[layer] = mm_tn(h, gb).astype(BF)

        gcur[...] = block_backward(
            gcur[...], xs[layer], wbuf.at[layer], dbuf.at[layer], qkv.at[layer],
            probs.at[layer], att.at[layer], mid.at[layer], pre.at[layer], dqkv,
            put_in, put_down,
        )
        for c in grad_copies(layer):
            c.start()
        return carry

    lax.fori_loop(0, layers, backward, 0)
    cut[...] = gcur[...].astype(BF)

    def slot_out(k):
        return pltpu.make_async_copy(
            cut.at[pl.ds(k * piece, piece)], back_ref.at[slot_ref[k]], slot_sem.at[k]
        )

    for k in range(capacity):
        @pl.when(k < filled)
        def _():
            slot_out(k).start()

    for k in range(capacity):
        @pl.when(k < filled)
        def _():
            slot_out(k).wait()

    for layer in range(layers):
        for c in grad_copies(layer):
            c.wait()


def greet_all(n, me):
    barrier = pltpu.get_barrier_semaphore()

    def greet(k, carry):
        pl.semaphore_signal(
            barrier, inc=1, device_id=(lax.rem(me + k, n),), device_id_type=MESH
        )
        return carry

    lax.fori_loop(1, n, greet, 0)
    pl.semaphore_wait(barrier, n - 1)


def exchange(n, me, source, target, send_sem, recv_sem, own_sem):
    own = pltpu.make_async_copy(source(me), target.at[me], own_sem)
    own.start()

    def remote(k):
        to = lax.rem(me + k, n)
        return pltpu.make_async_remote_copy(
            src_ref=source(to), dst_ref=target.at[me], send_sem=send_sem.at[k],
            recv_sem=recv_sem.at[k], device_id=(to,), device_id_type=MESH,
        )

    def start(k, carry):
        remote(k).start()
        return carry

    def finish(k, carry):
        remote(k).wait()
        return carry

    lax.fori_loop(1, n, start, 0)
    own.wait()
    lax.fori_loop(1, n, finish, 0)


def spread_kernel(n, group, cut_ref, out_ref, send_sem, recv_sem, own_sem):
    me = lax.axis_index("client")
    greet_all(n, me)
    exchange(
        n, me, lambda to: cut_ref.at[lax.rem(to, group)], out_ref, send_sem, recv_sem, own_sem
    )


def swap_kernel(n, in_ref, out_ref, send_sem, recv_sem, own_sem):
    me = lax.axis_index("client")
    greet_all(n, me)
    exchange(n, me, lambda to: in_ref.at[to], out_ref, send_sem, recv_sem, own_sem)


def total_kernel(n, in_ref, out_ref, got, send_sem, recv_sem, own_sem):
    me = lax.axis_index("client")
    greet_all(n, me)
    exchange(n, me, lambda to: in_ref.at[to], got, send_sem, recv_sem, own_sem)
    out_ref[...] = got[0].astype(F32)

    def add(k, carry):
        out_ref[...] += got[k].astype(F32)
        return carry

    lax.fori_loop(1, n, add, 0)


def vmem():
    return pl.BlockSpec(memory_space=pltpu.VMEM)


def smem():
    return pl.BlockSpec(memory_space=pltpu.SMEM)


def hbm():
    return pl.BlockSpec(memory_space=pl.ANY)


def comm_call(kernel, out, in_spec, out_spec, scratch, n, ident, arg):
    return pl.pallas_call(
        kernel,
        out_shape=out,
        in_specs=[in_spec],
        out_specs=out_spec,
        scratch_shapes=scratch
        + [
            pltpu.SemaphoreType.DMA((n,)),
            pltpu.SemaphoreType.DMA((n,)),
            pltpu.SemaphoreType.DMA,
        ],
        compiler_params=pltpu.CompilerParams(
            collective_id=ident, has_side_effects=True, vmem_limit_bytes=VMEM_LIMIT
        ),
    )(arg)


def shape(dims, kind):
    return jax.ShapeDtypeStruct(dims, kind)


def flip(block, bit):
    n = lax.axis_size("client")
    return lax.ppermute(block, "client", [(i, i ^ (1 << bit)) for i in range(n)])


def per_device(
    patches, labels, assign, patch_embed, positions, client_in, client_down,
    server_in, server_down, classifier,
):
    n = lax.axis_size("client")
    group = n // SHARDS
    bits = group.bit_length() - 1
    me = lax.axis_index("client")
    rank = me % group
    shard = me // group
    rows = patches.shape[0]
    width = client_in.shape[0]
    cols = client_in.shape[1]
    ff = client_down.shape[0]
    layers = server_in.shape[0]
    rows_in = server_in.shape[1]
    rows_down = server_down.shape[1]
    classes = classifier.shape[2]
    piece = rows // group
    per_image = IMG // group
    capacity = SLOTS * group
    s_rows = capacity * piece
    routes = assign.reshape(n)
    params = pltpu.CompilerParams(vmem_limit_bytes=VMEM_LIMIT)

    in_pieces = [server_in]
    down_pieces = [server_down]
    for bit in range(bits):
        in_pieces = in_pieces + [flip(p, bit) for p in in_pieces]
        down_pieces = down_pieces + [flip(p, bit) for p in down_pieces]

    def kept(r):
        return [
            shape((r, 3 * width), F32),
            shape((r // LANES * HEADS, LANES, LANES), BF),
            shape((r, width), BF),
            shape((r, width), F32),
            shape((r, ff), F32),
        ]

    cut, x0, *saved = pl.pallas_call(
        client_forward_kernel,
        out_shape=[shape((rows, width), BF), shape((rows, width), F32)] + kept(rows),
        in_specs=[vmem()] * 5,
        out_specs=[vmem()] * 7,
        compiler_params=params,
    )(patches, patch_embed, positions, client_in, client_down)

    arrived = comm_call(
        functools.partial(spread_kernel, n, group),
        shape((n, piece, width), BF), vmem(), hbm(), [], n, 1,
        cut.reshape(group, piece, width),
    )

    class_shard = jnp.pad(
        lax.dynamic_index_in_dim(classifier, shard, 0, keepdims=False),
        ((0, 0), (0, LANES - classes)),
    )
    part_in = shape((layers, rows_in, cols), BF)
    part_down = shape((layers, rows_down, width), BF)
    res = pl.pallas_call(
        functools.partial(server_kernel, n, group, layers, per_image, capacity, classes),
        out_shape=[
            shape((1, capacity * per_image), F32),
            shape((n, piece, width), BF),
            shape((width, LANES), BF),
        ]
        + [part_in] * group
        + [part_down] * group,
        in_specs=[smem(), smem(), hbm(), vmem()] + [hbm()] * (2 * group),
        out_specs=[vmem(), hbm(), vmem()] + [hbm()] * (2 * group),
        scratch_shapes=[
            pltpu.VMEM((layers, width, cols), BF),
            pltpu.VMEM((layers, ff, width), BF),
            pltpu.VMEM((layers, width, cols), BF),
            pltpu.VMEM((layers, ff, width), BF),
            pltpu.VMEM((layers + 1, s_rows, width), F32),
        ]
        + [pltpu.VMEM((layers,) + s.shape, s.dtype) for s in kept(s_rows)]
        + [
            pltpu.VMEM((s_rows, 3 * width), BF),
            pltpu.VMEM((s_rows, width), F32),
            pltpu.VMEM((s_rows, width), BF),
            pltpu.SMEM((capacity,), jnp.int32),
            pltpu.SemaphoreType.DMA((layers, 2 * group)),
            pltpu.SemaphoreType.DMA((layers, 2 * group)),
            pltpu.SemaphoreType.DMA((capacity,)),
        ],
        compiler_params=params,
    )(routes, labels, arrived, class_shard, *in_pieces, *down_pieces)
    losses, back, gclass = res[:3]
    parts_in = list(res[3 : 3 + group])
    parts_down = list(res[3 + group :])

    returned = comm_call(
        functools.partial(swap_kernel, n),
        shape((n, piece, width), BF), hbm(), hbm(), [], n, 2, back,
    )

    half = group // 2
    while half:
        bit = half.bit_length() - 1
        parts_in = [
            parts_in[i].astype(F32) + flip(parts_in[i + half].astype(BF), bit).astype(F32)
            for i in range(half)
        ]
        parts_down = [
            parts_down[i].astype(F32) + flip(parts_down[i + half].astype(BF), bit).astype(F32)
            for i in range(half)
        ]
        half //= 2
    gsum = gclass.astype(F32)
    for bit in range(bits):
        gsum = gsum + flip(gsum.astype(BF), bit).astype(F32)
    grad_class = lax.dynamic_slice_in_dim(gsum, rank * rows_in, rows_in, 0)[:, :classes]

    r_in = cols // n
    pack_rows = r_in + (ff // width + 1) * PAD
    packed = pl.pallas_call(
        functools.partial(client_backward_kernel, n, group),
        out_shape=shape((n, pack_rows, width), BF),
        in_specs=[smem(), hbm()] + [vmem()] * 9,
        out_specs=vmem(),
        scratch_shapes=[
            pltpu.VMEM((group, piece, width), BF),
            pltpu.VMEM((rows, 3 * width), BF),
            pltpu.SemaphoreType.DMA,
        ],
        compiler_params=params,
    )(routes, returned, patches, client_in, client_down, x0, *saved)

    summed = comm_call(
        functools.partial(total_kernel, n),
        shape((pack_rows, width), F32), vmem(), vmem(),
        [pltpu.VMEM((n, pack_rows, width), BF)], n, 3, packed,
    )
    own = width // n
    tail = summed[r_in:].reshape(ff // width + 1, PAD, width)[:, :own]
    grad_in = summed[:r_in].T
    grad_down = tail[:-1].transpose(0, 2, 1).reshape(ff, own)
    last = tail[-1].T
    patch = patches.shape[1]
    return (
        losses,
        last[:patch],
        last[width - LANES : width - LANES + TOK],
        grad_in,
        grad_down,
        parts_in[0],
        parts_down[0],
        grad_class,
    )


def solution(mesh):
    whole = P()
    in_specs = (
        P("client", None), whole, whole, whole, whole, whole, whole,
        P(None, "client", None), P(None, "client", None), whole,
    )
    out_specs = (
        P("client", None), P(None, "client"), P(None, "client"), P(None, "client"),
        P(None, "client"), P(None, "client", None), P(None, "client", None), P("client", None),
    )
    return jax.shard_map(
        per_device, mesh=mesh, in_specs=in_specs, out_specs=out_specs, check_vma=False
    )
```
